32 devices in a mesh: seg: 4 (over z), dev: 8 (over y, x, core).
Axes of the slice: x: 2, y: 2, z: 4, core: 2. Of those that a mesh axis runs over, the one named last changes fastest.
Arguments:
- positions: float32 [3, 4, 3072, 128], P(None, 'seg', 'dev'), may hold values from -6 to 6
- velocity: float32 [3, 4, 3072, 128], P(None, 'seg', 'dev'), may hold values from -6 to 6
- node_mass: bfloat16 [4, 3072, 128], P('seg', 'dev'), may hold values from 0.5 to 2
- stiffness: bfloat16 [4, 3072, 128], P('seg', 'dev'), may hold values from 0.25 to 2
- contact_patch: int32 [4, 8, 8], P('seg', 'dev'), may hold values from -1 to 2, as said below
- cross_patch: int32 [4, 8, 2], P('seg', 'dev'), may hold values from 0 to 2
Outputs:
- velocity_next: float32 [3, 4, 3072, 128], P(None, 'seg', 'dev')
The draws below stay inside these ranges and needn't reach their ends.
Inputs may be any that keep to these rules, and one draw needn't show every extreme that they name: `contact_patch`: entry [s, i, q] is -1 where runs i and q of segment s form no contact pair, else the number within run i of run i's patch in that pair; entry [s, i, q] is -1 exactly when entry [s, q, i] is; entries [s, i, i] are -1; in every segment some run has a pair with every other run. `cross_patch`: entry [s, i, 0] is the number within run i of the patch of segment s that meets run i of the next segment; entry [s, i, 1] the one that meets run i of the previous segment.
All inputs are finite; a program needn't handle non-finite values.
Results may differ from the reference program's by a relative error of at most 0.0028.
Values may be sent and summed in bfloat16 or wider, within the bound.
No kernel may reach another device: no remote copies, remote signals or barrier semaphores. Data moves between devices by JAX's collectives and lax.ppermute only.
A program may use at most 64 MiB of HBM per device.

```python
import math
import jax
import jax.numpy as jnp
import numpy as np
from jax import lax

P_DEV = 3
PATCH_ROWS = 128
COLS = 128
BAND = 4
SEGS = 4
RUNS = 8
STRIP = 3072


def draw_contact_patch(key, part):
    base = jax.random.fold_in(key, 7)
    key_links, key_hub, key_patch = jax.random.split(base, 3)
    coins = (jax.random.randint(key_links, (SEGS, RUNS, RUNS), 0, 5) >= 1).astype(jnp.int32)
    upper = jnp.triu(coins, 1)
    linked = upper + jnp.swapaxes(upper, 1, 2) > 0
    hub_run = jax.random.randint(key_hub, (SEGS, 1, 1), 0, RUNS)
    ranks = jnp.arange(RUNS)
    touching = (ranks[None, :, None] == hub_run) | (ranks[None, None, :] == hub_run)
    apart = ranks[:, None] != ranks[None, :]
    linked = (linked | touching) & apart[None]
    chosen = jax.random.randint(key_patch, (SEGS, RUNS, RUNS), 0, P_DEV)
    return jnp.where(linked, chosen, -1).astype(jnp.int32)


def set_ends(values, stream_key, smallest, high):
    place = [jax.random.randint(jax.random.fold_in(stream_key, axis), (), 0, length) for axis, length in enumerate(values.shape)]
    main_axis = values.shape.index(max(values.shape))
    neighbour = place[:main_axis] + [(place[main_axis] + 1) % values.shape[main_axis]] + place[main_axis + 1:]
    return values.at[tuple(place)].set(smallest).at[tuple(neighbour)].set(high)


def block_scale(stream_key, shape, shards, low, high):
    def one(dim, parts):
        steps = jax.random.uniform(jax.random.fold_in(jax.random.fold_in(stream_key, 6), dim), (parts,), jnp.float32, low / len(shards), high / len(shards))
        return jnp.repeat(jnp.exp(steps), shape[dim] // parts).reshape((-1,) + (1,) * (len(shape) - dim - 1))

    level = one(*shards[0])
    for cut in shards[1:]:
        level = level * one(*cut)
    return level


def normal_values(key, shape, scale, limit, cuts=(), held_as=jnp.bfloat16):
    drawn = scale * jax.random.normal(key, shape, jnp.float32)
    if cuts:
        drawn = drawn * block_scale(key, shape, cuts, -0.22, 0.18)
    return jnp.clip(drawn, -limit, limit).astype(held_as)


def setup_inputs(seed: int = 0) -> dict:
    keys = jax.random.split(jax.random.key(seed), 7)
    return {
        "positions": normal_values(keys[0], (3, SEGS, STRIP, COLS), 1.0, 6.0, ((1, 4), (2, 8)), jnp.float32),
        "velocity": normal_values(keys[1], (3, SEGS, STRIP, COLS), 1.0, 6.0, ((1, 4), (2, 8)), jnp.float32),
        "node_mass": jnp.clip(jnp.exp(math.log(2.0) - 1.3862944 * jax.random.uniform(keys[2], (SEGS, STRIP, COLS), jnp.float32) ** block_scale(keys[2], (SEGS, STRIP, COLS), ((0, 4), (1, 8)), -0.2, 0.2)), 0.5, 2.0).astype(jnp.bfloat16),
        "stiffness": jnp.clip(jnp.exp(math.log(2.0) - 2.0794415 * jax.random.uniform(keys[3], (SEGS, STRIP, COLS), jnp.float32) ** block_scale(keys[3], (SEGS, STRIP, COLS), ((0, 4), (1, 8)), -0.2, 0.2)), 0.25, 2.0).astype(jnp.bfloat16),
        "contact_patch": draw_contact_patch(jax.random.fold_in(keys[6], 71), 0),
        "cross_patch": set_ends(jax.random.randint(keys[5], (SEGS, RUNS, 2), 0, P_DEV), jax.random.fold_in(keys[5], 1), 0, P_DEV - 1).astype(jnp.int32),
    }


penalty = 1.5
reach_sq = 4.0
time_step = 0.2


def pair_forces(own_patch, other_patch):
    columns = own_patch.shape[-1]
    leading = [(0, 0)] * (own_patch.ndim - 1)
    padded = jnp.pad(other_patch, leading + [(BAND, BAND)])
    inside = jnp.pad(jnp.ones((columns,), jnp.float32), (BAND, BAND))
    force_own = jnp.zeros(own_patch.shape, jnp.float32)
    force_other = jnp.zeros(padded.shape, jnp.float32)
    for offset in range(2 * BAND + 1):
        facing = padded[..., offset:offset + columns]
        differ = own_patch - facing
        weight = penalty * jnp.exp(-jnp.sum(differ * differ, axis=-3, keepdims=True) / reach_sq) * inside[offset:offset + columns]
        pulled = weight * differ
        force_own = force_own + pulled
        force_other = force_other - jnp.pad(pulled, leading + [(offset, 2 * BAND - offset)])
    return force_own, force_other[..., BAND:BAND + columns]


def internal_force(positions, springs):
    still = (0, 0)
    row_flow = 0.5 * (springs[:, 1:] + springs[:, :-1]) * (positions[:, :, 1:] - positions[:, :, :-1])
    col_flow = 0.5 * (springs[:, :, 1:] + springs[:, :, :-1]) * (positions[..., 1:] - positions[..., :-1])
    total = jnp.pad(row_flow, (still, still, (0, 1), still)) - jnp.pad(row_flow, (still, still, (1, 0), still))
    total = total + jnp.pad(col_flow, (still, still, still, (0, 1))) - jnp.pad(col_flow, (still, still, still, (1, 0)))
    return total


def reference(positions, velocity, node_mass, stiffness, contact_patch, cross_patch):
    internal = internal_force(positions, stiffness.astype(jnp.float32))
    rounded = lax.optimization_barrier(positions.astype(jnp.bfloat16)).astype(jnp.float32)
    low_np, high_np = np.triu_indices(RUNS, 1)
    paired = len(low_np)
    seg_pairs = jnp.asarray(np.repeat(np.arange(SEGS), paired), dtype=jnp.int32)
    run_low = jnp.asarray(np.tile(low_np, SEGS), dtype=jnp.int32)
    run_high = jnp.asarray(np.tile(high_np, SEGS), dtype=jnp.int32)
    entry_low = contact_patch[seg_pairs, run_low, run_high]
    entry_high = contact_patch[seg_pairs, run_high, run_low]
    live_pairs = (entry_low >= 0).astype(jnp.float32)
    row_low = (run_low * P_DEV + jnp.maximum(entry_low, 0)) * PATCH_ROWS
    row_high = (run_high * P_DEV + jnp.maximum(entry_high, 0)) * PATCH_ROWS
    cross_seg = jnp.asarray(np.repeat(np.arange(SEGS), RUNS), dtype=jnp.int32)
    cross_run = jnp.asarray(np.tile(np.arange(RUNS), SEGS), dtype=jnp.int32)
    next_seg = (cross_seg + 1) % SEGS
    cross_low = (cross_run * P_DEV + cross_patch[cross_seg, cross_run, 0]) * PATCH_ROWS
    cross_high = (cross_run * P_DEV + cross_patch[next_seg, cross_run, 1]) * PATCH_ROWS
    items = (jnp.concatenate([seg_pairs, cross_seg]).astype(jnp.int32),
             jnp.concatenate([row_low, cross_low]).astype(jnp.int32),
             jnp.concatenate([seg_pairs, next_seg]).astype(jnp.int32),
             jnp.concatenate([row_high, cross_high]).astype(jnp.int32),
             jnp.concatenate([live_pairs, jnp.ones((SEGS * RUNS,), jnp.float32)]))
    extent = (3, 1, PATCH_ROWS, COLS)

    def visit(contact, item):
        seg_low, start_row_low, seg_high, start_row_high, live = item
        zero = jnp.zeros((), jnp.int32)
        start_low = (zero, seg_low, start_row_low, zero)
        start_high = (zero, seg_high, start_row_high, zero)
        low_patch = lax.dynamic_slice(rounded, start_low, extent)[:, 0]
        high_patch = lax.dynamic_slice(rounded, start_high, extent)[:, 0]
        force_low, force_high = pair_forces(low_patch, high_patch)
        current = lax.dynamic_slice(contact, start_low, extent)
        contact = lax.dynamic_update_slice(contact, current + live * force_low[:, None], start_low)
        current = lax.dynamic_slice(contact, start_high, extent)
        contact = lax.dynamic_update_slice(contact, current + live * force_high[:, None], start_high)
        return contact, None

    contact, _ = lax.scan(visit, jnp.zeros(positions.shape, jnp.float32), items)
    return velocity + time_step * (internal + contact) / node_mass.astype(jnp.float32)
```

```python
import functools
import math

import jax
import jax.numpy as jnp
from jax import lax
from jax.experimental import pallas as pl
from jax.experimental.pallas import tpu as pltpu
from jax.sharding import PartitionSpec as P

PATCH_ROWS = 128
BAND = 4
EXTRA = 8
CHUNK = 16

penalty = 1.5
reach_sq = 4.0
time_step = 0.2

root = math.sqrt(math.log2(math.e) / reach_sq)
FAR = -1.0e9

VMEM = pl.BlockSpec(memory_space=pltpu.VMEM)
SMEM = pl.BlockSpec(memory_space=pltpu.SMEM)


def patterns(n):
    if n & (n - 1) == 0:
        order = sorted(range(1, n), key=lambda k: (k & 1, -bin(k >> 1).count("1"), k))
        halo = [k for k in order if k & (k + 1) == 0]
        return order, halo, (lambda i, k: i ^ k), (lambda i, k: i ^ k)
    order = list(range(1, n))
    halo = sorted({1, n - 1})
    return order, halo, (lambda i, k: (i + k) % n), (lambda i, k: (i - k + n) % n)


def prepare_kernel(n, order, halo, target, table, cross, places, stiff, *outs):
    me = lax.axis_index("dev")
    rows = places.shape[2]

    def put(out, patch):
        start = pl.multiple_of(jnp.maximum(patch, 0) * PATCH_ROWS, PATCH_ROWS)
        for j in range(3):
            out[j, :PATCH_ROWS, :] = places[j, 0, pl.ds(start, PATCH_ROWS), :].astype(jnp.bfloat16)

    for k, out in zip(order, outs):
        put(out, table[0, 0, target(me, k)])
    put(outs[-2], cross[0, 0, 0])
    put(outs[-1], cross[0, 0, 1])
    for j in range(3):
        first = places[j, 0, 0:1, :]
        last = places[j, 0, rows - 1 : rows, :]
        parts = []
        for row in (first, last):
            high = row.astype(jnp.bfloat16).astype(jnp.float32)
            parts += [high, row - high]
        spring = stiff[0].astype(jnp.float32)
        parts += [spring[0:1, :], spring[rows - 1 : rows, :], first, first]
        block = jnp.concatenate(parts, axis=0).astype(jnp.bfloat16)
        for k, out in zip(order, outs):
            if k in halo:
                out[j, PATCH_ROWS:, :] = block


def strip_kernel(places, velocity, mass, stiff, base, inverse):
    rows, columns = places.shape[2:]
    step = 64
    lane = lax.broadcasted_iota(jnp.int32, (step, columns), 1)
    for r0 in range(0, rows, step):
        here = pl.ds(r0, step)
        spring = stiff[0, here, :].astype(jnp.float32)
        above = stiff[0, max(r0 - 16, 0) : max(r0 - 16, 0) + 16, :].astype(jnp.float32)[15:16]
        below = stiff[0, min(r0 + step, rows - 16) : min(r0 + step, rows - 16) + 16, :].astype(jnp.float32)[0:1]
        down = 0.5 * (spring + jnp.concatenate([spring[1:], below], axis=0))
        up = 0.5 * (spring + jnp.concatenate([above, spring[:-1]], axis=0))
        right = jnp.where(lane < columns - 1, 0.5 * (spring + pltpu.roll(spring, columns - 1, 1)), 0.0)
        scale = time_step / mass[0, here, :].astype(jnp.float32)
        inverse[here, :] = scale * (penalty / root)
        for j in range(3):
            x = places[j, 0, here, :]
            prev = places[j, 0, r0 - 1 : r0, :] if r0 else x[:1]
            after = places[j, 0, r0 + step : r0 + step + 1, :] if r0 + step < rows else x[step - 1 :]
            flow = down * (jnp.concatenate([x[1:], after], axis=0) - x)
            flow = flow + up * (jnp.concatenate([prev, x[:-1]], axis=0) - x)
            side = right * (pltpu.roll(x, columns - 1, 1) - x)
            flow = flow + side - pltpu.roll(side, 1, 1)
            base[j, here, :] = velocity[j, 0, here, :] + scale * flow


def reach_masks(columns):
    lane = lax.broadcasted_iota(jnp.int32, (CHUNK, columns), 1)
    masks = []
    for t in range(-BAND, BAND + 1):
        inside = (lane + t >= 0) & (lane + t < columns)
        masks.append(jnp.where(inside, 0.0, FAR).astype(jnp.float32))
    return masks


def add_pair(own, other, total, patch, masks):
    columns = total.shape[-1]
    for r0 in range(0, PATCH_ROWS, CHUNK):
        mine = [own[j, r0 : r0 + CHUNK, :].astype(jnp.float32) * root for j in range(3)]
        facing = [other[j, r0 : r0 + CHUNK, :].astype(jnp.float32) * root for j in range(3)]
        force = [None] * 3
        for t in range(-BAND, BAND + 1):
            shifted = [pltpu.roll(b, (-t) % columns, 1) if t else b for b in facing]
            d = [a - b for a, b in zip(mine, shifted)]
            square = d[0] * d[0] + d[1] * d[1] + d[2] * d[2]
            weight = jnp.exp2(masks[t + BAND] - square)
            pulled = [weight * v for v in d]
            force = [v if f is None else f + v for f, v in zip(force, pulled)]
        here = pl.ds(pl.multiple_of(patch * PATCH_ROWS + r0, CHUNK), CHUNK)
        for j in range(3):
            total[j, here, :] = total[j, here, :] + force[j]


def early_kernel(ks, target, table, *refs):
    me = lax.axis_index("dev")
    own, other, total = refs[: len(ks)], refs[len(ks) : 2 * len(ks)], refs[-1]
    masks = reach_masks(total.shape[-1])
    total[...] = jnp.zeros(total.shape, jnp.float32)
    for k, a, b in zip(ks, own, other):
        patch = table[0, 0, target(me, k)]

        @pl.when(patch >= 0)
        def _():
            add_pair(a, b, total, patch, masks)


def late_kernel(ks, n, halo, target, source, table, cross, places, stiff, base, inverse, early, *refs):
    me = lax.axis_index("dev")
    count = len(ks)
    own, other = refs[: count + 2], refs[count + 2 : 2 * count + 4]
    halos = refs[2 * count + 4 : 2 * count + 4 + len(halo)]
    out, total = refs[-2], refs[-1]
    rows, columns = places.shape[2:]
    masks = reach_masks(columns)
    total[...] = early[...]
    for k, a, b in zip(ks, own, other):
        patch = table[0, 0, target(me, k)]

        @pl.when(patch >= 0)
        def _():
            add_pair(a, b, total, patch, masks)

    for side in range(2):
        add_pair(own[count + side], other[count + side], total, cross[0, 0, side], masks)
    step = 64
    for r0 in range(0, rows, step):
        here = pl.ds(r0, step)
        for j in range(3):
            out[j, 0, here, :] = base[j, here, :] + inverse[here, :] * total[j, here, :]
    unit = root / penalty
    for k, block in zip(halo, halos):
        sender = source(me, k)
        for wanted, edge, at in ((me - 1, 0, 1), (me + 1, rows - 1, 0)):

            @pl.when(sender == wanted)
            def _():
                near = (edge // 16) * 16
                offset = edge - near
                spring = stiff[0, near : near + 16, :].astype(jnp.float32)[offset : offset + 1]
                scale = inverse[edge : edge + 1, :] * unit
                for j in range(3):
                    rows8 = block[j, PATCH_ROWS : PATCH_ROWS + EXTRA, :].astype(jnp.float32)
                    x = rows8[2 * at : 2 * at + 1] + rows8[2 * at + 1 : 2 * at + 2]
                    mean = 0.5 * (spring + rows8[4 + at : 5 + at])
                    flow = mean * (x - places[j, 0, edge : edge + 1, :])
                    out[j, 0, edge : edge + 1, :] = out[j, 0, edge : edge + 1, :] + scale * flow


def call(kernel, outs, operands, specs, flops, scratch=()):
    return pl.pallas_call(
        kernel,
        out_shape=outs,
        in_specs=specs,
        out_specs=[VMEM] * len(outs),
        scratch_shapes=list(scratch),
        cost_estimate=pl.CostEstimate(flops=flops, bytes_accessed=1 << 20, transcendentals=0),
    )(*operands)


def shards(positions, velocity, node_mass, stiffness, contact_patch, cross_patch):
    n = lax.axis_size("dev")
    segments = lax.axis_size("seg")
    rows, columns = positions.shape[2:]
    order, halo, target, source = patterns(n)
    shape = jax.ShapeDtypeStruct

    def packet(k):
        return shape((3, PATCH_ROWS + (EXTRA if k in halo else 0), columns), jnp.bfloat16)

    sent = call(
        functools.partial(prepare_kernel, n, order, halo, target),
        [packet(k) for k in order] + [packet(None)] * 2,
        (contact_patch, cross_patch, positions, stiffness),
        [SMEM, SMEM, VMEM, VMEM],
        1 << 20,
    )
    own = dict(zip(order, sent))
    next_patch, prev_patch = sent[-2:]
    got = {}
    program = [order[0]] + order[:0:-1]
    for k in program:
        route = [(i, target(i, k)) for i in range(n)]
        got[k] = lax.ppermute(own[k], "dev", route)
    from_next = lax.ppermute(prev_patch, "seg", [(i, (i - 1) % segments) for i in range(segments)])
    from_prev = lax.ppermute(next_patch, "seg", [(i, (i + 1) % segments) for i in range(segments)])
    field = shape((3, rows, columns), jnp.float32)
    base, inverse = call(
        strip_kernel,
        [field, shape((rows, columns), jnp.float32)],
        (positions, velocity, node_mass, stiffness),
        [VMEM] * 4,
        1 << 22,
    )
    half = len(order) // 2
    early_ks, late_ks = order[:half], order[half:]
    (early,) = call(
        functools.partial(early_kernel, early_ks, target),
        [field],
        [contact_patch] + [own[k] for k in early_ks] + [got[k] for k in early_ks],
        [SMEM] + [VMEM] * (2 * half),
        1 << 24,
    )
    mine = [own[k] for k in late_ks] + [next_patch, prev_patch]
    theirs = [got[k] for k in late_ks] + [from_next, from_prev]
    halos = [got[k] for k in halo]
    operands = [contact_patch, cross_patch, positions, stiffness, base, inverse, early]
    (out,) = call(
        functools.partial(late_kernel, late_ks, n, halo, target, source),
        [shape((3, 1, rows, columns), jnp.float32)],
        operands + mine + theirs + halos,
        [SMEM, SMEM] + [VMEM] * (5 + len(mine) + len(theirs) + len(halos)),
        1 << 24,
        [pltpu.VMEM((3, rows, columns), jnp.float32)],
    )
    return out


def solution(mesh):
    return jax.shard_map(
        shards,
        mesh=mesh,
        in_specs=(
            P(None, "seg", "dev", None),
            P(None, "seg", "dev", None),
            P("seg", "dev", None),
            P("seg", "dev", None),
            P("seg", "dev", None),
            P("seg", "dev", None),
        ),
        out_specs=P(None, "seg", "dev", None),
        check_vma=False,
    )
```

```python
import functools
import math

import jax
import jax.numpy as jnp
from jax import lax
from jax.experimental import pallas as pl
from jax.experimental.pallas import tpu as pltpu
from jax.sharding import PartitionSpec as P

PATCH_ROWS = 128
BAND = 4
EXTRA = 8
CHUNK = 16

penalty = 1.5
reach_sq = 4.0
time_step = 0.2

root = math.sqrt(math.log2(math.e) / reach_sq)
FAR = 1.0e4
PAD = 8
GRANT = 8 << 20

VMEM = pl.BlockSpec(memory_space=pltpu.VMEM)
HBM = pl.BlockSpec(memory_space=pltpu.HBM)
SMEM = pl.BlockSpec(memory_space=pltpu.SMEM)


def patterns(n):
    if n & (n - 1) == 0:
        order = sorted(range(1, n), key=lambda k: (k & 1, -bin(k >> 1).count("1"), k))
        halo = [k for k in order if k & (k + 1) == 0]
        return order, halo, (lambda i, k: i ^ k), (lambda i, k: i ^ k)
    order = list(range(1, n))
    halo = sorted({1, n - 1})
    return order, halo, (lambda i, k: (i + k) % n), (lambda i, k: (i - k + n) % n)


def prepare_kernel(n, order, halo, target, table_in, cross_in, places_in, stiff_in, *refs):
    count_out = len(order) + 2
    outs, (places, stiff, table_out, cross_out) = refs[:count_out], refs[count_out : count_out + 4]
    table, cross, turned, patch_sems, sems = refs[count_out + 4 :]
    me = lax.axis_index("dev")
    rows = places.shape[1]
    count = rows // PATCH_ROWS
    copies = []
    for p in range(count):
        here = pl.ds(p * PATCH_ROWS, PATCH_ROWS)
        copies.append(
            pltpu.make_async_copy(places_in.at[:, 0, here, :], places.at[:, here, :], patch_sems.at[p])
        )
    small = [
        pltpu.make_async_copy(table_in, table, sems.at[0]),
        pltpu.make_async_copy(cross_in, cross, sems.at[1]),
        pltpu.make_async_copy(stiff_in.at[0], stiff, sems.at[2]),
        pltpu.make_async_copy(table_in, table_out, sems.at[3]),
        pltpu.make_async_copy(cross_in, cross_out, sems.at[4]),
    ]
    for copy in small + copies:
        copy.start()
    for p in range(count):
        copies[p].wait()
        for j in range(3):
            block = places[j, p * PATCH_ROWS : (p + 1) * PATCH_ROWS, :]
            turned[p, j, :, :] = block.T.astype(jnp.bfloat16)
    for copy in small:
        copy.wait()
    columns = turned.shape[2]
    for k, out in zip(order, outs):
        patch = jnp.maximum(table[0, 0, target(me, k)], 0)
        out[:, :columns, :] = turned[patch]
    outs[-2][...] = turned[cross[0, 0, 0]]
    outs[-1][...] = turned[cross[0, 0, 1]]
    top = stiff[0:16, :].astype(jnp.float32)[0:1]
    bottom = stiff[rows - 16 : rows, :].astype(jnp.float32)[15:16]
    for j in range(3):
        first = places[j, 0:1, :]
        last = places[j, rows - 1 : rows, :]
        parts = []
        for row in (first, last):
            high = row.astype(jnp.bfloat16).astype(jnp.float32)
            parts += [high, row - high]
        parts += [top, bottom, first, first]
        block = jnp.concatenate(parts, axis=0).astype(jnp.bfloat16)
        for k, out in zip(order, outs):
            if k in halo:
                out[j, columns:, :] = block


def strip_kernel(places, velocity, mass, stiff, base, inverse):
    rows, columns = places.shape[1:]
    step = 64
    lane = lax.broadcasted_iota(jnp.int32, (step, columns), 1)
    for r0 in range(0, rows, step):
        here = pl.ds(r0, step)
        spring = stiff[here, :].astype(jnp.float32)
        above = stiff[max(r0 - 16, 0) : max(r0 - 16, 0) + 16, :].astype(jnp.float32)[15:16]
        below = stiff[min(r0 + step, rows - 16) : min(r0 + step, rows - 16) + 16, :].astype(jnp.float32)[0:1]
        down = 0.5 * (spring + jnp.concatenate([spring[1:], below], axis=0))
        up = 0.5 * (spring + jnp.concatenate([above, spring[:-1]], axis=0))
        right = jnp.where(lane < columns - 1, 0.5 * (spring + pltpu.roll(spring, columns - 1, 1)), 0.0)
        scale = time_step / mass[0, here, :].astype(jnp.float32)
        inverse[here, :] = scale * (penalty / root)
        for j in range(3):
            x = places[j, here, :]
            prev = places[j, r0 - 1 : r0, :] if r0 else x[:1]
            after = places[j, r0 + step : r0 + step + 1, :] if r0 + step < rows else x[step - 1 :]
            flow = down * (jnp.concatenate([x[1:], after], axis=0) - x)
            flow = flow + up * (jnp.concatenate([prev, x[:-1]], axis=0) - x)
            side = right * (pltpu.roll(x, columns - 1, 1) - x)
            flow = flow + side - pltpu.roll(side, 1, 1)
            base[j, here, :] = velocity[j, 0, here, :] + scale * flow


def add_pair(own, other, total, patch, facing):
    columns = total.shape[2]
    for c0 in range(0, columns, CHUNK):
        for j in range(3):
            block = other[j, c0 : c0 + CHUNK, :].astype(jnp.float32) * root
            facing[j, PAD + c0 : PAD + c0 + CHUNK, :] = block
    for c0 in range(0, columns, CHUNK):
        mine = [own[j, c0 : c0 + CHUNK, :].astype(jnp.float32) * root for j in range(3)]
        force = [None] * 3
        for t in range(-BAND, BAND + 1):
            d = [a - facing[j, PAD + c0 + t : PAD + c0 + t + CHUNK, :] for j, a in enumerate(mine)]
            weight = jnp.exp2(-(d[0] * d[0] + d[1] * d[1] + d[2] * d[2]))
            pulled = [weight * v for v in d]
            force = [v if f is None else f + v for f, v in zip(force, pulled)]
        for j in range(3):
            total[patch, j, c0 : c0 + CHUNK, :] = total[patch, j, c0 : c0 + CHUNK, :] + force[j]


def clear_pads(facing):
    rows = facing.shape[1]
    for j in range(3):
        far = jnp.full((PAD, facing.shape[2]), FAR, jnp.float32)
        facing[j, :PAD, :] = far
        facing[j, rows - PAD :, :] = far


def early_kernel(ks, target, table, *refs):
    me = lax.axis_index("dev")
    own, other = refs[: len(ks)], refs[len(ks) : 2 * len(ks)]
    total, facing = refs[-2:]
    clear_pads(facing)
    total[...] = jnp.zeros(total.shape, jnp.float32)
    for k, a, b in zip(ks, own, other):
        patch = table[0, 0, target(me, k)]

        @pl.when(patch >= 0)
        def _():
            add_pair(a, b, total, patch, facing)


def late_kernel(ks, n, halo, target, source, table, cross, places, stiff, base, inverse, early, *refs):
    me = lax.axis_index("dev")
    count = len(ks)
    own, other = refs[: count + 2], refs[count + 2 : 2 * count + 4]
    halos = refs[2 * count + 4 : 2 * count + 4 + len(halo)]
    out, total, facing = refs[-3:]
    rows, columns = places.shape[1:]
    clear_pads(facing)
    total[...] = early[...]
    for k, a, b in zip(ks, own, other):
        patch = table[0, 0, target(me, k)]

        @pl.when(patch >= 0)
        def _():
            add_pair(a, b, total, patch, facing)

    for side in range(2):
        add_pair(own[count + side], other[count + side], total, cross[0, 0, side], facing)
    for p in range(rows // PATCH_ROWS):
        here = pl.ds(p * PATCH_ROWS, PATCH_ROWS)
        for j in range(3):
            out[j, 0, here, :] = base[j, here, :] + inverse[here, :] * total[p, j, :, :].T
    unit = root / penalty
    for k, block in zip(halo, halos):
        sender = source(me, k)
        for wanted, edge, at in ((me - 1, 0, 1), (me + 1, rows - 1, 0)):

            @pl.when(sender == wanted)
            def _():
                near = (edge // 16) * 16
                offset = edge - near
                spring = stiff[near : near + 16, :].astype(jnp.float32)[offset : offset + 1]
                scale = inverse[edge : edge + 1, :] * unit
                for j in range(3):
                    rows8 = block[j, columns : columns + EXTRA, :].astype(jnp.float32)
                    x = rows8[2 * at : 2 * at + 1] + rows8[2 * at + 1 : 2 * at + 2]
                    mean = 0.5 * (spring + rows8[4 + at : 5 + at])
                    flow = mean * (x - places[j, edge : edge + 1, :])
                    out[j, 0, edge : edge + 1, :] = out[j, 0, edge : edge + 1, :] + scale * flow


def call(kernel, outs, operands, specs, flops, scratch=()):
    return pl.pallas_call(
        kernel,
        out_shape=outs,
        in_specs=specs,
        out_specs=[VMEM] * len(outs),
        scratch_shapes=list(scratch),
        compiler_params=pltpu.CompilerParams(vmem_limit_bytes=GRANT),
        cost_estimate=pl.CostEstimate(flops=flops, bytes_accessed=1 << 20, transcendentals=0),
    )(*operands)


def shards(positions, velocity, node_mass, stiffness, contact_patch, cross_patch):
    n = lax.axis_size("dev")
    segments = lax.axis_size("seg")
    rows, columns = positions.shape[2:]
    order, halo, target, source = patterns(n)
    shape = jax.ShapeDtypeStruct

    def packet(k):
        return shape((3, columns + (EXTRA if k in halo else 0), PATCH_ROWS), jnp.bfloat16)

    count = rows // PATCH_ROWS
    *sent, places, stiff, table, cross = call(
        functools.partial(prepare_kernel, n, order, halo, target),
        [packet(k) for k in order]
        + [packet(None)] * 2
        + [
            shape((3, rows, columns), jnp.float32),
            shape((rows, columns), jnp.bfloat16),
            shape(contact_patch.shape, jnp.int32),
            shape(cross_patch.shape, jnp.int32),
        ],
        [
            pltpu.with_memory_space_constraint(array, pltpu.HBM)
            for array in (contact_patch, cross_patch, positions, stiffness)
        ],
        [HBM] * 4,
        1 << 20,
        [
            pltpu.SMEM(contact_patch.shape, jnp.int32),
            pltpu.SMEM(cross_patch.shape, jnp.int32),
            pltpu.VMEM((count, 3, columns, PATCH_ROWS), jnp.bfloat16),
            pltpu.SemaphoreType.DMA((count,)),
            pltpu.SemaphoreType.DMA((5,)),
        ],
    )
    own = dict(zip(order, sent))
    next_patch, prev_patch = sent[-2:]
    got = {}
    program = [order[0]] + order[:0:-1]
    for k in program:
        route = [(i, target(i, k)) for i in range(n)]
        got[k] = lax.ppermute(own[k], "dev", route)
    from_next = lax.ppermute(prev_patch, "seg", [(i, (i - 1) % segments) for i in range(segments)])
    from_prev = lax.ppermute(next_patch, "seg", [(i, (i + 1) % segments) for i in range(segments)])
    forces = shape((count, 3, columns, PATCH_ROWS), jnp.float32)
    facing = pltpu.VMEM((3, columns + 2 * PAD, PATCH_ROWS), jnp.float32)
    field = shape((3, rows, columns), jnp.float32)
    base, inverse = call(
        strip_kernel,
        [field, shape((rows, columns), jnp.float32)],
        (places, velocity, node_mass, stiff),
        [VMEM] * 4,
        1 << 22,
    )
    half = len(order) // 2
    early_ks, late_ks = order[:half], order[half:]
    (early,) = call(
        functools.partial(early_kernel, early_ks, target),
        [forces],
        [table] + [own[k] for k in early_ks] + [got[k] for k in early_ks],
        [SMEM] + [VMEM] * (2 * half),
        1 << 24,
        [facing],
    )
    mine = [own[k] for k in late_ks] + [next_patch, prev_patch]
    theirs = [got[k] for k in late_ks] + [from_next, from_prev]
    halos = [got[k] for k in halo]
    operands = [table, cross, places, stiff, base, inverse, early]
    (out,) = call(
        functools.partial(late_kernel, late_ks, n, halo, target, source),
        [shape((3, 1, rows, columns), jnp.float32)],
        operands + mine + theirs + halos,
        [SMEM, SMEM] + [VMEM] * (5 + len(mine) + len(theirs) + len(halos)),
        1 << 24,
        [pltpu.VMEM(forces.shape, jnp.float32), facing],
    )
    return out


def solution(mesh):
    return jax.shard_map(
        shards,
        mesh=mesh,
        in_specs=(
            P(None, "seg", "dev", None),
            P(None, "seg", "dev", None),
            P("seg", "dev", None),
            P("seg", "dev", None),
            P("seg", "dev", None),
            P("seg", "dev", None),
        ),
        out_specs=P(None, "seg", "dev", None),
        check_vma=False,
    )
```
